32 devices in a mesh: row: 8 (over y, x, core), col: 4 (over z).
Axes of the slice: x: 2, y: 2, z: 4, core: 2. Of those that a mesh axis runs over, the one named last changes fastest.
Arguments:
- gradient: float32 [2048, 4608], P('row', 'col'), may hold values from -12 to 12
- first_moment: float32 [2048, 4608], P('row', 'col'), may hold values from -12 to 12, as said below
- second_moment: float32 [2048, 4608], P('row', 'col'), may hold values from 0.01 to 1
- weights: float32 [2048, 4608], P('row', 'col'), may hold values from -6 to 6
- eigenbasis: float32 [4608, 4608], P('row', 'col'), may hold values from -1 to 1, as said below
Outputs:
- new_weights: float32 [2048, 4608], P('row', 'col')
- new_first: float32 [2048, 4608], P('row', 'col')
- new_second: float32 [2048, 4608], P('row', 'col')
The draws below stay inside these ranges and needn't reach their ends.
Inputs may be any that keep to these rules, and one draw needn't show every extreme that they name: `first_moment`: every entry's magnitude is at most 12. eigenbasis is orthogonal: its columns are orthonormal.
All inputs are finite; a program needn't handle non-finite values.
Results may differ from the reference program's by a relative error of at most 0.000059.
Values sent between devices are 32-bit elements; how exact they have to be, the bound alone decides.
No kernel may reach another device: no remote copies, remote signals or barrier semaphores. Data moves between devices by JAX's collectives and lax.ppermute only.
A program may use at most 64 MiB of HBM per device.

```python
import math
import jax
import jax.numpy as jnp
from jax import lax

D = 4608
VOCAB = 2048


def draw_first_moment(key, part):
    key_rows = jax.random.fold_in(key, 11)
    key_cells = jax.random.fold_in(key, 12)
    row_factor = jnp.exp(jax.random.uniform(key_rows, (VOCAB, 1), jnp.float32, jnp.log(0.3), jnp.log(3.0)))
    cells = jax.random.truncated_normal(key_cells, -4.0, 4.0, (VOCAB, D), jnp.float32)
    return (cells * row_factor).astype(jnp.float32)


def draw_eigenbasis(key, part):
    key_basis = jax.random.fold_in(key, 21)
    source = jax.random.normal(key_basis, (D, D), jnp.float32)
    orthogonal, upper = jnp.linalg.qr(source)
    return orthogonal.astype(jnp.float32)


def steps_of(own_key, dims, cuts, least, largest):
    level = 1.0
    for position, shards_of in cuts:
        heights = jax.random.uniform(jax.random.fold_in(jax.random.fold_in(own_key, 6), position), (shards_of,), jnp.float32, least / len(cuts), largest / len(cuts))
        level = level * jnp.repeat(jnp.exp(heights), dims[position] // shards_of).reshape((-1,) + (1,) * (len(dims) - 1 - position))
    return level


def gaussian(stream_key, shape, spread, bound, split=(), dtype=jnp.bfloat16):
    drawn = spread * jax.random.normal(stream_key, shape, jnp.float32)
    if split:
        drawn = drawn * steps_of(stream_key, shape, split, -0.22, 0.18)
    return jnp.clip(drawn, -bound, bound).astype(dtype)


def setup_inputs(seed: int = 0) -> dict:
    keys = jax.random.split(jax.random.key(seed), 6)
    gradient = gaussian(keys[0], (VOCAB, D), 2.0, 12.0, ((0, 8), (1, 4)), jnp.float32)
    first_moment = draw_first_moment(jax.random.fold_in(keys[5], 71), 0)
    second_moment = jnp.clip(jnp.exp(math.log(1.0) - 4.6051702 * jax.random.uniform(keys[2], (VOCAB, D), jnp.float32) ** steps_of(keys[2], (VOCAB, D), ((0, 8), (1, 4)), -0.2, 0.2)), 0.01, 1.0)
    weights = gaussian(keys[3], (VOCAB, D), 1.0, 6.0, ((0, 8), (1, 4)), jnp.float32)
    eigenbasis = draw_eigenbasis(jax.random.fold_in(keys[5], 71), 0)
    return dict(gradient=gradient, first_moment=first_moment, second_moment=second_moment, weights=weights, eigenbasis=eigenbasis)


bias_first = 1.0 - 0.9 ** 10
bias_second = 1.0 - 0.999 ** 10
epsilon = 1e-08
step_rate = 0.25

def reference(gradient, first_moment, second_moment, weights, eigenbasis):
    highest = lax.Precision.HIGHEST
    rotated = jnp.dot(gradient.astype(jnp.float32), eigenbasis.astype(jnp.float32), precision=highest, preferred_element_type=jnp.float32)
    new_first = 0.9 * first_moment + 0.1 * rotated
    new_second = 0.999 * second_moment + 0.001 * rotated * rotated
    direction = new_first / bias_first / (jnp.sqrt(new_second / bias_second) + epsilon)
    row_rms = jnp.sqrt(lax.optimization_barrier(jnp.sum(direction * direction, axis=1, keepdims=True)) / D)
    update = jnp.dot(direction.astype(jnp.float32), eigenbasis.T.astype(jnp.float32), precision=highest, preferred_element_type=jnp.float32)
    new_weights = weights - step_rate * update / jnp.maximum(1.0, row_rms)
    return (new_weights, new_first, new_second)
```

```python
import jax
import jax.numpy as jnp
from jax import lax
from jax.experimental import pallas as pl
from jax.experimental.pallas import tpu as pltpu
from jax.sharding import PartitionSpec as P


bias_first = 1.0 - 0.9**10
bias_second = 1.0 - 0.999**10
epsilon = 1e-08
step_rate = 0.25


f32, bf16 = jnp.float32, jnp.bfloat16


def plain(gradient, first_moment, second_moment, weights, eigenbasis):
    high = lax.Precision.HIGH
    slab = lax.all_gather(eigenbasis, "row", axis=0, tiled=True)
    whole = lax.all_gather(gradient, "col", axis=1, tiled=True)
    rotated = jnp.dot(whole, slab, precision=high, preferred_element_type=f32)
    new_first = 0.9 * first_moment + 0.1 * rotated
    new_second = 0.999 * second_moment + 0.001 * rotated * rotated
    direction = new_first / bias_first / (jnp.sqrt(new_second / bias_second) + epsilon)
    sum_squares = lax.psum(jnp.sum(direction * direction, axis=1), "col")
    part = lax.dot_general(slab, direction, (((1,), (1,)), ((), ())), precision=high, preferred_element_type=f32)
    update = lax.psum_scatter(part, "col", scatter_dimension=0, tiled=True).T
    row_rms = jnp.sqrt(sum_squares / slab.shape[0])[:, None]
    new_weights = weights - step_rate * update / jnp.maximum(1.0, row_rms)
    return (new_weights, new_first, new_second)


def split(x):
    hi = x.astype(bf16)
    return hi, (x - hi.astype(f32)).astype(bf16)


def start_piece(pieces, r, core, slot, sem):
    half = slot.shape[0] // 2
    for rr, c, first, ref in pieces:
        if rr == r:
            at = pl.multiple_of(lax.rem(core + c, 2) * half + first, 8)
            pltpu.make_async_copy(ref, slot.at[pl.ds(at, ref.shape[0])], sem).start()


def start_block(grads, n, block, col, slot, sem):
    for s in range(1 - n, n):
        if grads[s] is not None:

            @pl.when(col - block == s)
            def _():
                first = 0
                for ref in grads[s]:
                    pltpu.make_async_copy(ref, slot.at[pl.ds(first, ref.shape[0])], sem).start()
                    first += ref.shape[0]


def landed(slot, sem):
    pltpu.make_async_copy(slot, slot, sem).wait()


def nt(a, b):
    return lax.dot_general(a, b, (((1,), (1,)), ((), ())), preferred_element_type=f32)


def by_distance(n, reach, refs):
    out = {s: None for s in range(1 - n, n)}
    out[0] = refs[:1]
    for s in range(1, reach + 1):
        out[s] = refs[2 * s - 1 : 2 * s + 1]
        out[-s] = refs[2 * (reach + s) - 1 : 2 * (reach + s) + 1]
    return out


def product(g, hi, lo):
    g_hi, g_lo = split(g)
    part = jnp.dot(g_hi, hi, preferred_element_type=f32)
    part += jnp.dot(g_hi, lo, preferred_element_type=f32)
    part += jnp.dot(g_lo, hi, preferred_element_type=f32)
    return part


def cut_of(width):
    return (width // 128 + 1) // 2 * 128


def mark_kernel(place, out):
    for k in range(place.shape[0]):
        out[k] = place[k]


def mark(place):
    return pl.pallas_call(
        mark_kernel,
        out_shape=jax.ShapeDtypeStruct(place.shape, place.dtype),
        in_specs=[SM],
        out_specs=SM,
        compiler_params=params(VMEM_MIB),
        cost_estimate=pl.CostEstimate(flops=1024, bytes_accessed=64, transcendentals=0),
    )(place)


def blocked(q_hi, q_lo, d_hi, d_lo):
    return nt(q_hi, d_hi) + nt(q_lo, d_hi) + nt(q_hi, d_lo)


def early_kernel(n, layout, place, *refs):
    count, reach = len(layout), n - 2
    grads = by_distance(n, reach, refs[: 4 * reach + 1])
    refs = refs[4 * reach + 1 :]
    pieces = [(*key, ref) for key, ref in zip(layout, refs[:count])]
    out, s_hi, s_lo, g_all, stage, hi, lo, g_sem, q_sem, out_sem = refs[count:]
    col, pair, core, skip = place[0], place[1], place[2], place[3]
    steps = n - 1

    def fetch(t):
        slot = t % 2
        r = jnp.where(t == 0, skip, jnp.where(t - 1 < skip, t - 1, t))
        if t > 0:
            start_block(grads, n, pair ^ r, col, g_all.at[slot], g_sem.at[slot])
        for k in range(n - 1):

            @pl.when(r == k)
            def _():
                start_piece(pieces, k, core, stage.at[slot], q_sem.at[slot])

    fetch(0)
    fetch(1)
    landed(stage.at[0], q_sem.at[0])
    hi[...], lo[...] = split(stage[0])
    sent = [pltpu.make_async_copy(x, y, out_sem.at[k]) for k, (x, y) in enumerate(((hi, s_hi), (lo, s_lo)))]
    for copy in sent:
        copy.start()
    for t in range(1, steps):
        slot = t % 2
        if t + 1 < steps:
            fetch(t + 1)
        landed(stage.at[slot], q_sem.at[slot])
        landed(g_all.at[slot], g_sem.at[slot])
        part = product(g_all[slot], *split(stage[slot]))
        if t == 1:
            out[...] = part
        else:
            out[...] += part
    for copy in sent:
        copy.wait()


def middle_kernel(n, place, *refs):
    reach = n - 1
    grads = by_distance(n, reach, refs[: 4 * reach + 1])
    acc, s_hi, s_lo, out, r_hi, r_lo, g_all, held, q_hi, q_lo, g_sem, q_sem, out_sem = refs[4 * reach + 1 :]
    col, pair, skip = place[0], place[1], place[3]
    brought = [pltpu.make_async_copy(x, y, q_sem.at[k]) for k, (x, y) in enumerate(((s_hi, q_hi), (s_lo, q_lo), (acc, held)))]
    start_block(grads, n, pair ^ skip, col, g_all.at[0], g_sem.at[0])
    for copy in brought:
        copy.start()
    start_block(grads, n, pair ^ (n - 1), col, g_all.at[1], g_sem.at[1])
    landed(g_all.at[0], g_sem.at[0])
    g_hi, g_lo = split(g_all[0])
    brought[0].wait()
    part = jnp.dot(g_hi, q_hi[...], preferred_element_type=f32)
    part += jnp.dot(g_lo, q_hi[...], preferred_element_type=f32)
    brought[1].wait()
    part += jnp.dot(g_hi, q_lo[...], preferred_element_type=f32)
    brought[2].wait()
    held[...] += part
    sent = pltpu.make_async_copy(held, out, out_sem)
    sent.start()
    landed(g_all.at[1], g_sem.at[1])
    r_hi[...], r_lo[...] = split(g_all[1])
    sent.wait()


def rotate_kernel(n, layout, place, *refs):
    count = len(layout)
    pieces = [(*key, ref) for key, ref in zip(layout, refs[:count])]
    given, refs = refs[count : count + 7], refs[count + 7 :]
    made, refs = refs[:5], refs[5:]
    held, refs = refs[:7], refs[7:]
    acc, g_hi, g_lo, first, second, s_hi, s_lo = held
    results, (stage, q_hi, q_lo, p_sem, in_sem, out_sem) = refs[:5], refs[5:]
    nf, ns, d, top, bottom = results
    core, lead = place[2], place[4]
    half, last = stage.shape[1], n - 1
    for _, c, start, ref in pieces:
        pltpu.make_async_copy(ref, stage.at[c, pl.ds(start, ref.shape[0])], p_sem.at[c]).start()
    brought = [pltpu.make_async_copy(x, y, in_sem.at[k]) for k, (x, y) in enumerate(zip(given, held))]
    for copy in brought[1:3]:
        copy.start()
    for c in range(2):
        landed(stage.at[c], p_sem.at[c])
        if c:
            for k in (0, 3, 4):
                brought[k].start()

            @pl.when(lead != last)
            def _():
                brought[5].start()
                brought[6].start()

        at = pl.multiple_of(lax.rem(core + c, 2) * half, 16)
        q_hi[pl.ds(at, half)], q_lo[pl.ds(at, half)] = split(stage[c])
    for copy in brought[1:3]:
        copy.wait()
    total = jnp.dot(g_hi[...], q_hi[...], preferred_element_type=f32)
    total += jnp.dot(g_hi[...], q_lo[...], preferred_element_type=f32)
    total += jnp.dot(g_lo[...], q_hi[...], preferred_element_type=f32)
    for k in (0, 3, 4):
        brought[k].wait()
    total += acc[...]
    nf[...] = 0.9 * first[...] + 0.1 * total
    ns[...] = 0.999 * second[...] + 0.001 * total * total
    d[...] = nf[...] / bias_first / (jnp.sqrt(ns[...] / bias_second) + epsilon)
    sent = [pltpu.make_async_copy(x, y, out_sem.at[k]) for k, (x, y) in enumerate(zip(results, made))]
    for copy in sent[:3]:
        copy.start()
    d_hi, d_lo = split(d[...])
    cut = top.shape[0] - 8
    ones = jnp.ones((8, d.shape[1]), bf16)
    hi, rest = split(d[...] * d[...])
    top[cut:] = nt(ones, hi) + nt(ones, rest)

    def put(a, b):
        u = blocked(a[...], b[...], d_hi, d_lo)
        top[:cut] = u[:cut]
        bottom[...] = u[cut:]

    @pl.when(lead == last)
    def _():
        put(q_hi, q_lo)

    @pl.when(lead != last)
    def _():
        brought[5].wait()
        brought[6].wait()
        put(s_hi, s_lo)

    sent[3].start()
    sent[4].start()
    for copy in sent:
        copy.wait()


ANY = pl.BlockSpec(memory_space=pl.ANY)
VM = pl.BlockSpec(memory_space=pltpu.VMEM)
SM = pl.BlockSpec(memory_space=pltpu.SMEM)


VMEM_MIB = 44


def params(mib):
    return pltpu.CompilerParams(vmem_limit_bytes=mib * 2**20)


def cost(products, rows, width):
    return pl.CostEstimate(flops=int(6 * products * rows * width * width), bytes_accessed=8 * width * width, transcendentals=0)


def early(place, grads, keys, pieces, n):
    rows, width = grads[0].shape
    shape = jax.ShapeDtypeStruct
    return pl.pallas_call(
        lambda *refs: early_kernel(n, keys, *refs),
        out_shape=[shape((rows, width), f32)] + [shape((width, width), bf16)] * 2,
        in_specs=[SM] + [ANY] * (len(grads) + len(pieces)),
        out_specs=[VM, ANY, ANY],
        scratch_shapes=[
            pltpu.VMEM((2, rows, width), f32),
            pltpu.VMEM((2, width, width), f32),
            pltpu.VMEM((width, width), bf16),
            pltpu.VMEM((width, width), bf16),
        ]
        + [pltpu.SemaphoreType.DMA((2,))] * 3,
        compiler_params=params(VMEM_MIB),
        cost_estimate=cost(n - 2, rows, width),
        name="early",
    )(place, *grads, *pieces)


def middle(place, grads, acc, s_hi, s_lo, n):
    rows, width = acc.shape
    shape = jax.ShapeDtypeStruct
    return pl.pallas_call(
        lambda *refs: middle_kernel(n, *refs),
        out_shape=[shape((rows, width), f32)] + [shape((rows, width), bf16)] * 2,
        in_specs=[SM] + [ANY] * (len(grads) + 3),
        out_specs=[ANY] + [VM] * 2,
        scratch_shapes=[pltpu.VMEM((2, rows, width), f32), pltpu.VMEM((rows, width), f32)]
        + [pltpu.VMEM((width, width), bf16)] * 2
        + [pltpu.SemaphoreType.DMA((2,)), pltpu.SemaphoreType.DMA((3,)), pltpu.SemaphoreType.DMA],
        compiler_params=params(VMEM_MIB),
        cost_estimate=cost(1, rows, width),
        name="middle",
    )(place, *grads, acc, s_hi, s_lo)


def rotate(place, keys, pieces, given, n):
    rows, width = given[0].shape
    half, cut = width // 2, cut_of(width)
    shape = jax.ShapeDtypeStruct
    return pl.pallas_call(
        lambda *refs: rotate_kernel(n, keys, *refs),
        out_shape=[shape((rows, width), f32)] * 3 + [shape((cut + 8, rows), f32), shape((width - cut, rows), f32)],
        in_specs=[SM] + [ANY] * (len(pieces) + len(given)),
        out_specs=[ANY] * 5,
        scratch_shapes=[pltpu.VMEM(x.shape, x.dtype) for x in given]
        + [pltpu.VMEM((rows, width), f32)] * 3
        + [pltpu.VMEM((cut + 8, rows), f32), pltpu.VMEM((width - cut, rows), f32)]
        + [pltpu.VMEM((2, half, width), f32)]
        + [pltpu.VMEM((width, width), bf16)] * 2
        + [pltpu.SemaphoreType.DMA((k,)) for k in (2, len(given), 5)],
        compiler_params=params(VMEM_MIB),
        cost_estimate=cost(2, rows, width),
        name="rotate",
    )(place, *pieces, *given)


def back_kernel(n, layout, place, *refs):
    count = len(layout)
    direction, top, bottom = refs[0:3]
    pieces = [(*key, ref) for key, ref in zip(layout, refs[3 : 3 + count])]
    outs, (stage, u, q_sem) = refs[3 + count : -3], refs[-3:]
    col, pair, core, lead = place[0], place[1], place[2], place[4]
    for r in range(min(2, n)):
        start_piece(pieces, r, core, stage.at[r % 2], q_sem.at[r % 2])
    hi, lo = split(direction[...])
    cut = top.shape[0] - 8

    @pl.loop(0, n)
    def _(r):
        slot = lax.rem(r, 2)
        landed(stage.at[slot], q_sem.at[slot])
        block = pair ^ r
        step = jnp.where(block > col, n - 1 - block + col, block + n - 1 - col)
        spot = jnp.where(block == col, 2 * n - 4, jnp.where(block > col, step - 1, n - 3 + step))

        @pl.when(r != lead)
        def _():
            u[...] = blocked(*split(stage[slot]), hi, lo)

        @pl.when(r == lead)
        def _():
            u[:cut] = top[:cut]
            u[cut:] = bottom[...]

        for k in range(2, n):

            @pl.when(r + 2 == k)
            def _():
                start_piece(pieces, k, core, stage.at[k % 2], q_sem.at[k % 2])

        for k in range(2 * n - 3):

            @pl.when((spot == k) & ((block == col) | (step > 0)))
            def _():
                outs[2 * k][:cut] = u[:cut]
                outs[2 * k][cut:] = top[cut:]
                outs[2 * k + 1][...] = u[cut:]


def back(place, direction, top, bottom, keys, pieces, n):
    rows, width = direction.shape
    cut = cut_of(width)
    shapes = [jax.ShapeDtypeStruct((cut + 8, rows), f32), jax.ShapeDtypeStruct((width - cut, rows), f32)]
    return pl.pallas_call(
        lambda *refs: back_kernel(n, keys, *refs),
        out_shape=shapes * (2 * n - 3),
        in_specs=[SM] + [VM] * 3 + [ANY] * len(pieces),
        out_specs=[VM] * (4 * n - 6),
        scratch_shapes=[pltpu.VMEM((2, width, width), f32), pltpu.VMEM((width, rows), f32), pltpu.SemaphoreType.DMA((2,))],
        compiler_params=params(VMEM_MIB),
        cost_estimate=pl.CostEstimate(flops=6 * rows * width * width * (n - 1), bytes_accessed=4 * n * width * width, transcendentals=0),
        name="back",
    )(place, direction, top, bottom, *pieces)


def finish_top_kernel(deep, weights, a0, a1, a2, out, norm, held, sem):
    cut = held.shape[1]
    total = a0[...] + a1[...] + a2[...]
    norm[...] = jnp.maximum(1.0, jnp.sqrt(total[cut:] / deep))
    held[...] = weights[:, :cut] - (step_rate * total[:cut] / norm[:1]).T
    copy = pltpu.make_async_copy(held, out.at[:, pl.ds(0, cut)], sem)
    copy.start()
    copy.wait()


def finish_bottom_kernel(weights, norm, b0, b1, b2, _, out, held, sem):
    cut = weights.shape[1] - held.shape[1]
    total = b0[...] + b1[...] + b2[...]
    held[...] = weights[:, cut:] - (step_rate * total / norm[:1]).T
    copy = pltpu.make_async_copy(held, out.at[:, pl.ds(cut, held.shape[1])], sem)
    copy.start()
    copy.wait()


def finish(weights, parts, deep):
    rows, width = weights.shape
    cut = cut_of(width)
    shape = jax.ShapeDtypeStruct(weights.shape, f32)
    some, norm = pl.pallas_call(
        lambda *refs: finish_top_kernel(deep, *refs),
        out_shape=[shape, jax.ShapeDtypeStruct((8, rows), f32)],
        in_specs=[VM] * 4,
        out_specs=[ANY, VM],
        scratch_shapes=[pltpu.VMEM((rows, cut), f32), pltpu.SemaphoreType.DMA],
        compiler_params=params(VMEM_MIB),
        cost_estimate=cost(0.1, rows, width),
        name="finish_top",
    )(weights, *parts[:3])
    return pl.pallas_call(
        finish_bottom_kernel,
        out_shape=shape,
        in_specs=[VM] * 5 + [ANY],
        out_specs=ANY,
        scratch_shapes=[pltpu.VMEM((rows, width - cut), f32), pltpu.SemaphoreType.DMA],
        input_output_aliases={5: 0},
        compiler_params=params(VMEM_MIB),
        cost_estimate=cost(0.1, rows, width),
        name="finish_bottom",
    )(weights, norm, *parts[3:], some)


def swapped(n_row, bit):
    return [(i, i ^ bit) for i in range(n_row)]


def gather_basis(q, n_row):
    bits = []
    bit = 2
    while bit < n_row:
        bits.append(bit)
        bit *= 2
    half = q.shape[0] // 2
    keys, arrays = [], []

    def put(r, start, x):
        keys.append((r, 0, start))
        arrays.append(x)
        keys.append((r, 1, start))
        arrays.append(lax.ppermute(x, "row", swapped(n_row, 1)))

    put(0, 0, q)
    for start, order, x in ((0, bits, q[:half]), (half, bits[::-1], q[half:])):
        held = [(0, x)]
        for b in order:
            fresh = [(r | (b // 2), lax.ppermute(v, "row", swapped(n_row, b))) for r, v in held]
            for r, v in fresh:
                put(r, start, v)
            held += fresh
    return keys, arrays


def gather_line(g, n):
    rights, lefts = [], []
    half = g.shape[0] // 2
    a = b = [g[:half], g[half:]]
    for s in range(1, n):
        right = [(i, i + 1) for i in range(s - 1, n - 1)]
        left = [(i, i - 1) for i in range(n - s, 0, -1)]
        a = [lax.ppermute(x, "col", right) for x in a]
        b = [lax.ppermute(x, "col", left) for x in b]
        rights += a
        lefts += b
    return rights, lefts


def scatter_line(parts, blocks, n):
    got = [[None, None] for _ in parts]
    for s in range(n - 1):
        for h, part in enumerate(parts):
            for way in (0, 1):
                load = part if s == 0 else blocks[2 * (way * (n - 2) + s - 1) + h] + got[h][way]
                perm = [(i, i + 1) for i in range(s + 1)] if way == 0 else [(i, i - 1) for i in range(n - 1 - s, n)]
                got[h][way] = lax.ppermute(load, "col", perm)
    return [x for h in range(len(parts)) for x in (blocks[2 * (2 * n - 4) + h], *got[h])]


def solution(mesh):
    n_row, n_col = mesh.shape["row"], mesh.shape["col"]
    pairs = n_row // 2
    meets = n_row == 2 * n_col and pairs & (pairs - 1) == 0 and n_col > 2

    def per_device(gradient, first_moment, second_moment, weights, eigenbasis):
        width, n = gradient.shape[1], n_col
        if not (meets and width % 128 == 0 and eigenbasis.shape[0] % 32 == 0 and gradient.shape[0] % 16 == 0):
            return plain(gradient, first_moment, second_moment, weights, eigenbasis)
        row, col = lax.axis_index("row"), lax.axis_index("col")
        pair = row // 2
        end = (col == 0) | (col == n - 1)
        lead = jnp.where(end, pair ^ (n - 1 - col), n - 1)
        skip = jnp.where(lead == n - 1, 0, lead)
        place = jnp.stack([col, pair, row % 2, skip, lead]).astype(jnp.int32)
        keys, pieces = gather_basis(eigenbasis, n_row)
        rights, lefts = gather_line(gradient, n)
        place = mark(place)

        def some(wanted):
            return [key for key in keys if wanted(key)], [x for key, x in zip(keys, pieces) if wanted(key)]

        acc, s_hi, s_lo = early(place, [gradient, *rights[: 2 * n - 4], *lefts[: 2 * n - 4]], *some(lambda key: key[0] < n - 1), n)
        acc, g_hi, g_lo = middle(place, [gradient, *rights, *lefts], acc, s_hi, s_lo, n)
        given = [acc, g_hi, g_lo, first_moment, second_moment, s_hi, s_lo]
        new_first, new_second, direction, top, bottom = rotate(place, *some(lambda key: key[0] == n - 1), given, n)
        blocks = back(place, direction, top, bottom, keys, pieces, n)
        new_weights = finish(weights, scatter_line([top, bottom], blocks, n), width * n)
        return (new_weights, new_first, new_second)

    spec = P("row", "col")
    return jax.shard_map(per_device, mesh=mesh, in_specs=(spec,) * 5, out_specs=(spec,) * 3, check_vma=False)
```

```python
import jax
import jax.numpy as jnp
from jax import lax
from jax.experimental import pallas as pl
from jax.experimental.pallas import tpu as pltpu
from jax.sharding import PartitionSpec as P


bias_first = 1.0 - 0.9**10
bias_second = 1.0 - 0.999**10
epsilon = 1e-08
step_rate = 0.25


f32, bf16 = jnp.float32, jnp.bfloat16


def plain(gradient, first_moment, second_moment, weights, eigenbasis):
    high = lax.Precision.HIGH
    slab = lax.all_gather(eigenbasis, "row", axis=0, tiled=True)
    whole = lax.all_gather(gradient, "col", axis=1, tiled=True)
    rotated = jnp.dot(whole, slab, precision=high, preferred_element_type=f32)
    new_first = 0.9 * first_moment + 0.1 * rotated
    new_second = 0.999 * second_moment + 0.001 * rotated * rotated
    direction = new_first / bias_first / (jnp.sqrt(new_second / bias_second) + epsilon)
    sum_squares = lax.psum(jnp.sum(direction * direction, axis=1), "col")
    part = lax.dot_general(slab, direction, (((1,), (1,)), ((), ())), precision=high, preferred_element_type=f32)
    update = lax.psum_scatter(part, "col", scatter_dimension=0, tiled=True).T
    row_rms = jnp.sqrt(sum_squares / slab.shape[0])[:, None]
    new_weights = weights - step_rate * update / jnp.maximum(1.0, row_rms)
    return (new_weights, new_first, new_second)


def split(x):
    hi = x.astype(bf16)
    return hi, (x - hi.astype(f32)).astype(bf16)


def start_piece(pieces, r, core, slot, sem):
    half = slot.shape[0] // 2
    for rr, c, first, ref in pieces:
        if rr == r:
            at = pl.multiple_of(lax.rem(core + c, 2) * half + first, 8)
            pltpu.make_async_copy(ref, slot.at[pl.ds(at, ref.shape[0])], sem).start()


def start_block(grads, n, block, col, slot, sem):
    for s in range(1 - n, n):
        if grads[s] is not None:

            @pl.when(col - block == s)
            def _():
                first = 0
                for ref in grads[s]:
                    pltpu.make_async_copy(ref, slot.at[pl.ds(first, ref.shape[0])], sem).start()
                    first += ref.shape[0]


def landed(slot, sem):
    pltpu.make_async_copy(slot, slot, sem).wait()


def nt(a, b):
    return lax.dot_general(a, b, (((1,), (1,)), ((), ())), preferred_element_type=f32)


def by_distance(n, reach, refs):
    out = {s: None for s in range(1 - n, n)}
    out[0] = refs[:1]
    for s in range(1, reach + 1):
        out[s] = refs[2 * s - 1 : 2 * s + 1]
        out[-s] = refs[2 * (reach + s) - 1 : 2 * (reach + s) + 1]
    return out


def product(g, hi, lo):
    g_hi, g_lo = split(g)
    part = jnp.dot(g_hi, hi, preferred_element_type=f32)
    part += jnp.dot(g_hi, lo, preferred_element_type=f32)
    part += jnp.dot(g_lo, hi, preferred_element_type=f32)
    return part


def cut_of(width):
    return (width // 128 + 1) // 2 * 128


def mark_kernel(place, out):
    for k in range(place.shape[0]):
        out[k] = place[k]


def mark(place):
    return pl.pallas_call(
        mark_kernel,
        out_shape=jax.ShapeDtypeStruct(place.shape, place.dtype),
        in_specs=[SM],
        out_specs=SM,
        compiler_params=params(VMEM_MIB),
        cost_estimate=pl.CostEstimate(flops=1024, bytes_accessed=64, transcendentals=0),
    )(place)


def blocked(q_hi, q_lo, d_hi, d_lo):
    return nt(q_hi, d_hi) + nt(q_lo, d_hi) + nt(q_hi, d_lo)


def early_kernel(n, layout, place, *refs):
    count, reach = len(layout), n - 2
    grads = by_distance(n, reach, refs[: 4 * reach + 1])
    refs = refs[4 * reach + 1 :]
    pieces = [(*key, ref) for key, ref in zip(layout, refs[:count])]
    out, s_hi, s_lo, g_all, stage, hi, lo, g_sem, q_sem, out_sem = refs[count:]
    col, pair, core, skip = place[0], place[1], place[2], place[3]
    steps = n - 1

    def fetch(t):
        slot = t % 2
        r = jnp.where(t == 0, skip, jnp.where(t - 1 < skip, t - 1, t))
        if t > 0:
            start_block(grads, n, pair ^ r, col, g_all.at[slot], g_sem.at[slot])
        for k in range(n - 1):

            @pl.when(r == k)
            def _():
                start_piece(pieces, k, core, stage.at[slot], q_sem.at[slot])

    fetch(0)
    fetch(1)
    landed(stage.at[0], q_sem.at[0])
    hi[...], lo[...] = split(stage[0])
    sent = [pltpu.make_async_copy(x, y, out_sem.at[k]) for k, (x, y) in enumerate(((hi, s_hi), (lo, s_lo)))]
    for copy in sent:
        copy.start()
    for t in range(1, steps):
        slot = t % 2
        if t + 1 < steps:
            fetch(t + 1)
        landed(stage.at[slot], q_sem.at[slot])
        landed(g_all.at[slot], g_sem.at[slot])
        part = product(g_all[slot], *split(stage[slot]))
        if t == 1:
            out[...] = part
        else:
            out[...] += part
    for copy in sent:
        copy.wait()


def middle_kernel(n, place, *refs):
    reach = n - 1
    grads = by_distance(n, reach, refs[: 4 * reach + 1])
    s_hi, s_lo, out, r_hi, r_lo, g_all, held, q_hi, q_lo, g_sem, q_sem, out_sem = refs[4 * reach + 1 :]
    col, pair, skip = place[0], place[1], place[3]
    brought = [pltpu.make_async_copy(x, y, q_sem.at[k]) for k, (x, y) in enumerate(((s_hi, q_hi), (s_lo, q_lo)))]
    start_block(grads, n, pair ^ skip, col, g_all.at[0], g_sem.at[0])
    for copy in brought:
        copy.start()
    start_block(grads, n, pair ^ (n - 1), col, g_all.at[1], g_sem.at[1])
    landed(g_all.at[0], g_sem.at[0])
    g_hi, g_lo = split(g_all[0])
    brought[0].wait()
    part = jnp.dot(g_hi, q_hi[...], preferred_element_type=f32)
    part += jnp.dot(g_lo, q_hi[...], preferred_element_type=f32)
    brought[1].wait()
    part += jnp.dot(g_hi, q_lo[...], preferred_element_type=f32)
    held[...] = part
    sent = pltpu.make_async_copy(held, out, out_sem)
    sent.start()
    landed(g_all.at[1], g_sem.at[1])
    r_hi[...], r_lo[...] = split(g_all[1])
    sent.wait()


def rotate_kernel(n, layout, place, *refs):
    count = len(layout)
    pieces = [(*key, ref) for key, ref in zip(layout, refs[:count])]
    given, refs = refs[count : count + 8], refs[count + 8 :]
    made, refs = refs[:5], refs[5:]
    held, refs = refs[:8], refs[8:]
    part, g_hi, g_lo, first, second, s_hi, s_lo, acc = held
    results, (stage, q_hi, q_lo, p_sem, in_sem, out_sem) = refs[:5], refs[5:]
    nf, ns, d, top, bottom = results
    core, lead = place[2], place[4]
    half, last = stage.shape[1], n - 1
    for _, c, start, ref in pieces:
        pltpu.make_async_copy(ref, stage.at[c, pl.ds(start, ref.shape[0])], p_sem.at[c]).start()
    brought = [pltpu.make_async_copy(x, y, in_sem.at[k]) for k, (x, y) in enumerate(zip(given, held))]
    for copy in brought[1:3]:
        copy.start()
    for c in range(2):
        landed(stage.at[c], p_sem.at[c])
        if c:
            for k in (0, 3, 4, 7):
                brought[k].start()

            @pl.when(lead != last)
            def _():
                brought[5].start()
                brought[6].start()

        at = pl.multiple_of(lax.rem(core + c, 2) * half, 16)
        q_hi[pl.ds(at, half)], q_lo[pl.ds(at, half)] = split(stage[c])
    for copy in brought[1:3]:
        copy.wait()
    total = jnp.dot(g_hi[...], q_hi[...], preferred_element_type=f32)
    total += jnp.dot(g_hi[...], q_lo[...], preferred_element_type=f32)
    total += jnp.dot(g_lo[...], q_hi[...], preferred_element_type=f32)
    for k in (0, 3, 4, 7):
        brought[k].wait()
    total += acc[...] + part[...]
    nf[...] = 0.9 * first[...] + 0.1 * total
    ns[...] = 0.999 * second[...] + 0.001 * total * total
    d[...] = nf[...] / bias_first / (jnp.sqrt(ns[...] / bias_second) + epsilon)
    sent = [pltpu.make_async_copy(x, y, out_sem.at[k]) for k, (x, y) in enumerate(zip(results, made))]
    for copy in sent[:3]:
        copy.start()
    d_hi, d_lo = split(d[...])
    cut = top.shape[0] - 8
    ones = jnp.ones((8, d.shape[1]), bf16)
    hi, rest = split(d[...] * d[...])
    top[cut:] = nt(ones, hi) + nt(ones, rest)

    def put(a, b):
        u = blocked(a[...], b[...], d_hi, d_lo)
        top[:cut] = u[:cut]
        bottom[...] = u[cut:]

    @pl.when(lead == last)
    def _():
        put(q_hi, q_lo)

    @pl.when(lead != last)
    def _():
        brought[5].wait()
        brought[6].wait()
        put(s_hi, s_lo)

    sent[3].start()
    sent[4].start()
    for copy in sent:
        copy.wait()


ANY = pl.BlockSpec(memory_space=pl.ANY)
VM = pl.BlockSpec(memory_space=pltpu.VMEM)
SM = pl.BlockSpec(memory_space=pltpu.SMEM)


VMEM_MIB = 44


def params(mib):
    return pltpu.CompilerParams(vmem_limit_bytes=mib * 2**20)


def cost(products, rows, width):
    return pl.CostEstimate(flops=int(6 * products * rows * width * width), bytes_accessed=8 * width * width, transcendentals=0)


def early(place, grads, keys, pieces, n):
    rows, width = grads[0].shape
    shape = jax.ShapeDtypeStruct
    return pl.pallas_call(
        lambda *refs: early_kernel(n, keys, *refs),
        out_shape=[shape((rows, width), f32)] + [shape((width, width), bf16)] * 2,
        in_specs=[SM] + [ANY] * (len(grads) + len(pieces)),
        out_specs=[VM, ANY, ANY],
        scratch_shapes=[
            pltpu.VMEM((2, rows, width), f32),
            pltpu.VMEM((2, width, width), f32),
            pltpu.VMEM((width, width), bf16),
            pltpu.VMEM((width, width), bf16),
        ]
        + [pltpu.SemaphoreType.DMA((2,))] * 3,
        compiler_params=params(VMEM_MIB),
        cost_estimate=cost(n - 2, rows, width),
        name="early",
    )(place, *grads, *pieces)


def middle(place, grads, s_hi, s_lo, n):
    rows, width = grads[0].shape
    shape = jax.ShapeDtypeStruct
    return pl.pallas_call(
        lambda *refs: middle_kernel(n, *refs),
        out_shape=[shape((rows, width), f32)] + [shape((rows, width), bf16)] * 2,
        in_specs=[SM] + [ANY] * (len(grads) + 2),
        out_specs=[ANY] + [VM] * 2,
        scratch_shapes=[pltpu.VMEM((2, rows, width), f32), pltpu.VMEM((rows, width), f32)]
        + [pltpu.VMEM((width, width), bf16)] * 2
        + [pltpu.SemaphoreType.DMA((2,))] * 2 + [pltpu.SemaphoreType.DMA],
        compiler_params=params(VMEM_MIB),
        cost_estimate=cost(1, rows, width),
        name="middle",
    )(place, *grads, s_hi, s_lo)


def rotate(place, keys, pieces, given, n):
    rows, width = given[0].shape
    half, cut = width // 2, cut_of(width)
    shape = jax.ShapeDtypeStruct
    return pl.pallas_call(
        lambda *refs: rotate_kernel(n, keys, *refs),
        out_shape=[shape((rows, width), f32)] * 3 + [shape((cut + 8, rows), f32), shape((width - cut, rows), f32)],
        in_specs=[SM] + [ANY] * (len(pieces) + len(given)),
        out_specs=[ANY] * 5,
        scratch_shapes=[pltpu.VMEM(x.shape, x.dtype) for x in given]
        + [pltpu.VMEM((rows, width), f32)] * 3
        + [pltpu.VMEM((cut + 8, rows), f32), pltpu.VMEM((width - cut, rows), f32)]
        + [pltpu.VMEM((2, half, width), f32)]
        + [pltpu.VMEM((width, width), bf16)] * 2
        + [pltpu.SemaphoreType.DMA((k,)) for k in (2, len(given), 5)],
        compiler_params=params(VMEM_MIB),
        cost_estimate=cost(2, rows, width),
        name="rotate",
    )(place, *pieces, *given)


def back_kernel(n, layout, place, *refs):
    count = len(layout)
    direction, top, bottom = refs[0:3]
    pieces = [(*key, ref) for key, ref in zip(layout, refs[3 : 3 + count])]
    outs, (stage, u, q_sem) = refs[3 + count : -3], refs[-3:]
    col, pair, core, lead = place[0], place[1], place[2], place[4]
    for r in range(min(2, n)):
        start_piece(pieces, r, core, stage.at[r % 2], q_sem.at[r % 2])
    hi, lo = split(direction[...])
    cut = top.shape[0] - 8

    @pl.loop(0, n)
    def _(r):
        slot = lax.rem(r, 2)
        landed(stage.at[slot], q_sem.at[slot])
        block = pair ^ r
        step = jnp.where(block > col, n - 1 - block + col, block + n - 1 - col)
        spot = jnp.where(block == col, 2 * n - 4, jnp.where(block > col, step - 1, n - 3 + step))

        @pl.when(r != lead)
        def _():
            u[...] = blocked(*split(stage[slot]), hi, lo)

        @pl.when(r == lead)
        def _():
            u[:cut] = top[:cut]
            u[cut:] = bottom[...]

        for k in range(2, n):

            @pl.when(r + 2 == k)
            def _():
                start_piece(pieces, k, core, stage.at[k % 2], q_sem.at[k % 2])

        for k in range(2 * n - 3):

            @pl.when((spot == k) & ((block == col) | (step > 0)))
            def _():
                outs[2 * k][:cut] = u[:cut]
                outs[2 * k][cut:] = top[cut:]
                outs[2 * k + 1][...] = u[cut:]


def back(place, direction, top, bottom, keys, pieces, n):
    rows, width = direction.shape
    cut = cut_of(width)
    shapes = [jax.ShapeDtypeStruct((cut + 8, rows), f32), jax.ShapeDtypeStruct((width - cut, rows), f32)]
    return pl.pallas_call(
        lambda *refs: back_kernel(n, keys, *refs),
        out_shape=shapes * (2 * n - 3),
        in_specs=[SM] + [VM] * 3 + [ANY] * len(pieces),
        out_specs=[VM] * (4 * n - 6),
        scratch_shapes=[pltpu.VMEM((2, width, width), f32), pltpu.VMEM((width, rows), f32), pltpu.SemaphoreType.DMA((2,))],
        compiler_params=params(VMEM_MIB),
        cost_estimate=pl.CostEstimate(flops=6 * rows * width * width * (n - 1), bytes_accessed=4 * n * width * width, transcendentals=0),
        name="back",
    )(place, direction, top, bottom, *pieces)


def finish_top_kernel(deep, weights, a0, a1, a2, out, norm, held, sem):
    cut = held.shape[1]
    total = a0[...] + a1[...] + a2[...]
    norm[...] = jnp.maximum(1.0, jnp.sqrt(total[cut:] / deep))
    held[...] = weights[:, :cut] - (step_rate * total[:cut] / norm[:1]).T
    copy = pltpu.make_async_copy(held, out.at[:, pl.ds(0, cut)], sem)
    copy.start()
    copy.wait()


def finish_bottom_kernel(weights, norm, b0, b1, b2, _, out, held, sem):
    cut = weights.shape[1] - held.shape[1]
    total = b0[...] + b1[...] + b2[...]
    held[...] = weights[:, cut:] - (step_rate * total / norm[:1]).T
    copy = pltpu.make_async_copy(held, out.at[:, pl.ds(cut, held.shape[1])], sem)
    copy.start()
    copy.wait()


def finish(weights, parts, deep):
    rows, width = weights.shape
    cut = cut_of(width)
    shape = jax.ShapeDtypeStruct(weights.shape, f32)
    some, norm = pl.pallas_call(
        lambda *refs: finish_top_kernel(deep, *refs),
        out_shape=[shape, jax.ShapeDtypeStruct((8, rows), f32)],
        in_specs=[VM] * 4,
        out_specs=[ANY, VM],
        scratch_shapes=[pltpu.VMEM((rows, cut), f32), pltpu.SemaphoreType.DMA],
        compiler_params=params(VMEM_MIB),
        cost_estimate=cost(0.1, rows, width),
        name="finish_top",
    )(weights, *parts[:3])
    return pl.pallas_call(
        finish_bottom_kernel,
        out_shape=shape,
        in_specs=[VM] * 5 + [ANY],
        out_specs=ANY,
        scratch_shapes=[pltpu.VMEM((rows, width - cut), f32), pltpu.SemaphoreType.DMA],
        input_output_aliases={5: 0},
        compiler_params=params(VMEM_MIB),
        cost_estimate=cost(0.1, rows, width),
        name="finish_bottom",
    )(weights, norm, *parts[3:], some)


def swapped(n_row, bit):
    return [(i, i ^ bit) for i in range(n_row)]


def gather_basis(q, n_row):
    bits = []
    bit = 2
    while bit < n_row:
        bits.append(bit)
        bit *= 2
    half = q.shape[0] // 2
    keys, arrays = [], []

    def put(r, start, x):
        keys.append((r, 0, start))
        arrays.append(x)
        keys.append((r, 1, start))
        arrays.append(lax.ppermute(x, "row", swapped(n_row, 1)))

    put(0, 0, q)
    for start, order, x in ((0, bits, q[:half]), (half, bits[::-1], q[half:])):
        held = [(0, x)]
        for b in order:
            fresh = [(r | (b // 2), lax.ppermute(v, "row", swapped(n_row, b))) for r, v in held]
            for r, v in fresh:
                put(r, start, v)
            held += fresh
    return keys, arrays


def gather_line(g, n):
    rights, lefts = [], []
    half = g.shape[0] // 2
    a = b = [g[:half], g[half:]]
    for s in range(1, n):
        right = [(i, i + 1) for i in range(s - 1, n - 1)]
        left = [(i, i - 1) for i in range(n - s, 0, -1)]
        a = [lax.ppermute(x, "col", right) for x in a]
        b = [lax.ppermute(x, "col", left) for x in b]
        rights += a
        lefts += b
    return rights, lefts


def scatter_line(parts, blocks, n):
    got = [[None, None] for _ in parts]
    for s in range(n - 1):
        for h, part in enumerate(parts):
            for way in (0, 1):
                load = part if s == 0 else blocks[2 * (way * (n - 2) + s - 1) + h] + got[h][way]
                perm = [(i, i + 1) for i in range(s + 1)] if way == 0 else [(i, i - 1) for i in range(n - 1 - s, n)]
                got[h][way] = lax.ppermute(load, "col", perm)
    return [x for h in range(len(parts)) for x in (blocks[2 * (2 * n - 4) + h], *got[h])]


def solution(mesh):
    n_row, n_col = mesh.shape["row"], mesh.shape["col"]
    pairs = n_row // 2
    meets = n_row == 2 * n_col and pairs & (pairs - 1) == 0 and n_col > 2

    def per_device(gradient, first_moment, second_moment, weights, eigenbasis):
        width, n = gradient.shape[1], n_col
        if not (meets and width % 128 == 0 and eigenbasis.shape[0] % 32 == 0 and gradient.shape[0] % 16 == 0):
            return plain(gradient, first_moment, second_moment, weights, eigenbasis)
        row, col = lax.axis_index("row"), lax.axis_index("col")
        pair = row // 2
        end = (col == 0) | (col == n - 1)
        lead = jnp.where(end, pair ^ (n - 1 - col), n - 1)
        skip = jnp.where(lead == n - 1, 0, lead)
        place = jnp.stack([col, pair, row % 2, skip, lead]).astype(jnp.int32)
        keys, pieces = gather_basis(eigenbasis, n_row)
        rights, lefts = gather_line(gradient, n)
        place = mark(place)

        def some(wanted):
            return [key for key in keys if wanted(key)], [x for key, x in zip(keys, pieces) if wanted(key)]

        acc, s_hi, s_lo = early(place, [gradient, *rights[: 2 * n - 4], *lefts[: 2 * n - 4]], *some(lambda key: key[0] < n - 1), n)
        part, g_hi, g_lo = middle(place, [gradient, *rights, *lefts], s_hi, s_lo, n)
        given = [part, g_hi, g_lo, first_moment, second_moment, s_hi, s_lo, acc]
        new_first, new_second, direction, top, bottom = rotate(place, *some(lambda key: key[0] == n - 1), given, n)
        blocks = back(place, direction, top, bottom, keys, pieces, n)
        new_weights = finish(weights, scatter_line([top, bottom], blocks, n), width * n)
        return (new_weights, new_first, new_second)

    spec = P("row", "col")
    return jax.shard_map(per_device, mesh=mesh, in_specs=(spec,) * 5, out_specs=(spec,) * 3, check_vma=False)
```
